32 devices in a mesh: dp: 4 (over y, x), blk: 8 (over z, core).
Axes of the slice: x: 2, y: 2, z: 4, core: 2. Of those that a mesh axis runs over, the one named last changes fastest.
Arguments:
- particles: float32 [1024, 1024], P('blk'), may hold values from -14 to 14
- data_rows: bfloat16 [16384, 1024], P('dp'), may hold values from -0.1875 to 0.1875
- labels: int32 [16384], P('dp'), may hold values from 0 to 1
Outputs:
- descent: float32 [1024, 1024], P('blk')
The draws below stay inside these ranges and needn't reach their ends.
All inputs are finite; a program needn't handle non-finite values.
Results may differ from the reference program's by a relative error of at most 0.0045.
Values may be sent and summed in bfloat16 or wider, within the bound.
A program may use at most 64 MiB of HBM per device.

```python
import math
import jax
import jax.numpy as jnp
from jax import lax

D = 1024
PB = 128
M = 16384
N_BLK = 8


def draw_particles(key, part):
    row_total = PB * N_BLK
    sub_keys = jax.random.split(jax.random.fold_in(key, 4711), 4)
    cluster_total = 64
    centres = jax.random.truncated_normal(sub_keys[0], -4.0, 4.0, (cluster_total, D), jnp.float32)
    member = jax.random.randint(sub_keys[1], (row_total,), 0, cluster_total)
    scales = jnp.exp(jax.random.uniform(sub_keys[2], (cluster_total, 1), jnp.float32, jnp.log(0.5), jnp.log(3.0)))
    jitter = 0.3 * jax.random.truncated_normal(sub_keys[3], -4.0, 4.0, (row_total, D), jnp.float32)
    placed = (scales * centres)[member]
    return (placed + jitter).astype(jnp.float32)


def touch_ends(drawn, rng, low, high):
    spot = [jax.random.randint(jax.random.fold_in(rng, axis), (), 0, length) for axis, length in enumerate(drawn.shape)]
    widest = drawn.shape.index(max(drawn.shape))
    neighbour = spot[:widest] + [(spot[widest] + 1) % drawn.shape[widest]] + spot[widest + 1:]
    return drawn.at[tuple(spot)].set(low).at[tuple(neighbour)].set(high)


def shard_levels(key, dims, shards, smallest, largest):
    gain, own = 1.0, jax.random.fold_in(key, 6)
    for axis_at, parts in shards:
        heights = jnp.exp(jax.random.uniform(jax.random.fold_in(own, axis_at), (parts,), jnp.float32, smallest / len(shards), largest / len(shards)))
        gain = gain * jnp.repeat(heights, dims[axis_at] // parts).reshape([-1 if axis == axis_at else 1 for axis in range(len(dims))])
    return gain


def scatter_about(own_key, extent, scale, limit, cuts=(), dtype=jnp.bfloat16):
    factor_of = shard_levels(own_key, extent, cuts, -0.22, 0.18) if cuts else 1.0
    values = jax.random.normal(own_key, extent, jnp.float32) * scale * factor_of
    return jnp.minimum(jnp.maximum(values, -limit), limit).astype(dtype)


def setup_inputs(seed: int = 0) -> dict:
    key_list = jax.random.split(jax.random.key(seed), 4)
    particles = draw_particles(jax.random.fold_in(key_list[3], 71), 0)
    data_rows = scatter_about(key_list[1], (M, D), D ** -0.5, 0.1875, ((0, 4),))
    labels = touch_ends(jax.random.randint(key_list[2], (M,), 0, 2), jax.random.fold_in(key_list[2], 1), 0, 1).astype(jnp.int32)
    return {"particles": particles, "data_rows": data_rows, "labels": labels}


prior_var = 4.0


def pair_sums(left_x, left_s, right_x, right_s, inv_band):
    feature_count = left_x.shape[1]
    left_xf = left_x.astype(jnp.float32)
    left_sf = left_s.astype(jnp.float32)
    right_xf = right_x.astype(jnp.float32)
    right_sf = right_s.astype(jnp.float32)
    left_norm = jnp.sum(left_xf * left_xf, axis=1)
    right_norm = jnp.sum(right_xf * right_xf, axis=1)
    left_sx = jnp.sum(left_sf * left_xf, axis=1)
    right_sx = jnp.sum(right_sf * right_xf, axis=1)
    gram_xx = jnp.einsum("id,jd->ij", left_x, right_x, preferred_element_type=jnp.float32)
    gram_ss = jnp.einsum("id,jd->ij", left_s, right_s, preferred_element_type=jnp.float32)
    cross_dot = jnp.einsum("id,jd->ij", jnp.concatenate([left_x, left_s], axis=1),
                           jnp.concatenate([right_s, right_x], axis=1), preferred_element_type=jnp.float32)
    distance = left_norm[:, None] + right_norm[None, :] - 2.0 * gram_xx
    kernel = jnp.exp(-0.5 * inv_band * distance)
    bracket = (gram_ss + inv_band * (left_sx[:, None] - cross_dot + right_sx[None, :])
               + feature_count * inv_band - inv_band * inv_band * distance)
    weighted_kernel = kernel * bracket
    kernel_sum = jnp.sum(kernel, axis=1)
    weighted_sum = jnp.sum(weighted_kernel, axis=1)
    both_rows = jnp.dot(kernel.astype(jnp.bfloat16), jnp.concatenate([right_x, right_s], axis=1),
                        preferred_element_type=jnp.float32)
    kernel_x = both_rows[:, :feature_count]
    kernel_s = both_rows[:, feature_count:]
    weighted_x = jnp.dot(weighted_kernel.astype(jnp.bfloat16), right_x, preferred_element_type=jnp.float32)
    return (kernel_sum, weighted_sum, kernel_x, kernel_s, weighted_x)


def forces(left_x, left_s, sums, inv_band, particle_count):
    kernel_sum, weighted_sum, kernel_x, kernel_s, weighted_x = sums
    left_xf = left_x.astype(jnp.float32)
    left_sf = left_s.astype(jnp.float32)
    spread = kernel_sum[:, None] * left_xf - kernel_x
    score_force = (kernel_s + inv_band * spread) / particle_count
    place_force = (-inv_band * (weighted_sum[:, None] * left_xf - weighted_x)
                   + inv_band * (kernel_sum[:, None] * left_sf - kernel_s)
                   - 2.0 * inv_band * inv_band * spread) / particle_count
    return score_force, place_force


def reference(particles, data_rows, labels):
    particle_count, feature_count = particles.shape
    inv_band = 1.0 / feature_count
    block_rows = math.gcd(particle_count, 512)
    block_count = particle_count // block_rows
    label_vals = labels.astype(jnp.float32)
    x_low = particles.astype(jnp.bfloat16)
    stacked_x = x_low.reshape(block_count, block_rows, feature_count)
    stacked_p = particles.reshape(block_count, block_rows, feature_count)

    def score_block(pieces):
        x_block, p_block = pieces
        logits = jnp.einsum("pd,md->pm", x_block, data_rows, preferred_element_type=jnp.float32)
        probability = jax.nn.sigmoid(logits)
        residual = (label_vals[None, :] - probability).astype(jnp.bfloat16)
        return jnp.dot(residual, data_rows, preferred_element_type=jnp.float32) - p_block / prior_var

    scores = lax.map(score_block, (stacked_x, stacked_p)).reshape(particle_count, feature_count)
    s_low = scores.astype(jnp.bfloat16)
    stacked_s = s_low.reshape(block_count, block_rows, feature_count)

    def descent_block(pieces):
        x_block, s_block = pieces
        sums = pair_sums(x_block, s_block, x_low, s_low, inv_band)
        score_force, place_force = forces(x_block, s_block, sums, inv_band, particle_count)
        logits = jnp.einsum("pd,md->pm", x_block, data_rows, preferred_element_type=jnp.float32)
        probability = jax.nn.sigmoid(logits)
        curvature = probability * (1.0 - probability)
        projected = jnp.einsum("pd,md->pm", score_force.astype(jnp.bfloat16), data_rows,
                               preferred_element_type=jnp.float32)
        weighted_rows = (curvature * projected).astype(jnp.bfloat16)
        data_term = jnp.dot(weighted_rows, data_rows, preferred_element_type=jnp.float32)
        return data_term - place_force + score_force / prior_var

    return lax.map(descent_block, (stacked_x, stacked_s)).reshape(particle_count, feature_count)
```

```python
import functools

import jax
import jax.numpy as jnp
from jax import lax
from jax.experimental import pallas as pl
from jax.experimental.pallas import tpu as pltpu
from jax.sharding import PartitionSpec as P

MESH = pl.DeviceIdType.MESH
prior_var = 4.0
f32 = jnp.float32
bf16 = jnp.bfloat16
CORES = 2
CHUNKS = 4
TILES = 8


def dot_nn(a, b):
    return jnp.dot(a, b, preferred_element_type=f32)


def dot_nt(a, b):
    return lax.dot_general(a, b, (((1,), (1,)), ((), ())), preferred_element_type=f32)


def remote(src, dst, send, recv, device):
    return pltpu.make_async_remote_copy(
        src_ref=src, dst_ref=dst, send_sem=send, recv_sem=recv, device_id=device, device_id_type=MESH
    )


def kernel(
    n, nb, part_ref, lab_ref, data_hbm, out_ref,
    data, curv, rows_low, x_low, x_all, s_all, s_own, psf, kx, ks, g_own, g_all, o_all,
    s_out, g_out, o_out, s_in, g_in, o_in,
    load_sem, xz, xf, sr, sa, sz, sf, gr, ga, orr, oa,
):
    rows, width = part_ref.shape
    share = rows // n
    nz = nb // CORES
    cw = width // CHUNKS
    tile = data_hbm.shape[0] // TILES
    total = rows * nb
    pairs = share * nb
    c_band = 1.0 / width
    dp = lax.axis_index("dp")
    blk = lax.axis_index("blk")
    zi, core = blk // CORES, lax.rem(blk, CORES)
    own = pl.ds(pl.multiple_of(dp * share, share), share)
    mine = pl.ds(pl.multiple_of(blk * share, share), share)
    partner = (dp, zi * CORES + 1 - core)

    def dp_dev(p):
        return lax.rem(dp + p, n)

    def z_dev(q):
        return lax.rem(zi + q, nz) * CORES + core

    def share_of(index):
        return pl.ds(pl.multiple_of(index * share, share), share)

    def load(t):
        piece = pl.ds(t * tile, tile)
        return pltpu.make_async_copy(data_hbm.at[piece], data.at[piece], load_sem.at[t])

    for t in range(TILES):
        load(t).start()

    barrier = pltpu.get_barrier_semaphore()
    for p in range(1, n):
        pl.semaphore_signal(barrier, inc=1, device_id=(dp_dev(p), blk), device_id_type=MESH)
    for q in range(1, nz):
        pl.semaphore_signal(barrier, inc=1, device_id=(dp, z_dev(q)), device_id_type=MESH)
    pl.semaphore_signal(barrier, inc=1, device_id=partner, device_id_type=MESH)
    x_low[...] = part_ref[...].astype(bf16)
    x_all[mine, :] = part_ref[own, :].astype(bf16)
    pl.semaphore_wait(barrier, n - 1 + nz - 1 + 1)

    sent = []

    def go(copy):
        copy.start()
        sent.append(copy)

    def arrived(place, sems, index, device):
        remote(place, place, sems[0].at[index], sems[1].at[index], device).wait_recv()

    for q in range(1, nz):
        go(remote(x_all.at[mine], x_all.at[mine], xz[0].at[q - 1], xz[1].at[q - 1], (dp, z_dev(q))))
    go(remote(x_all.at[mine], x_all.at[mine], xf[0].at[0], xf[1].at[0], partner))

    def logit_step(t, carry):
        piece = pl.ds(pl.multiple_of(t * tile, tile), tile)
        load(t).wait()
        probability = jax.nn.sigmoid(dot_nt(x_low[...], data[piece, :]))
        curv[:, piece] = probability * (1.0 - probability)
        rows_low[:, piece] = (lab_ref[:, piece].astype(f32) - probability).astype(bf16)
        return carry

    lax.fori_loop(0, TILES, logit_step, 0)

    for q in range(1, nz):
        slot = share_of(lax.rem(zi + nz - q, nz) * CORES + core)
        arrived(x_all.at[slot], xz, q - 1, partner)
        go(remote(x_all.at[slot], x_all.at[slot], xf[0].at[q], xf[1].at[q], partner))

    def scatter(c, buffer, landing, sems):
        for p in range(1, n):
            to = dp_dev(p)
            go(remote(buffer.at[c, share_of(to)], landing.at[c, p - 1],
                      sems[0].at[c, p - 1], sems[1].at[c, p - 1], (to, blk)))

    def reduced(c, landing, sems):
        value = psf[c, own, :]
        for p in range(1, n):
            arrived(landing.at[c, p - 1], sems, (c, p - 1), partner)
            value = value + landing[c, p - 1].astype(f32)
        return value

    def gather(c, buffer, sems):
        for p in range(1, n):
            go(remote(buffer.at[c, own], buffer.at[c, own],
                      sems[0].at[c, p - 1], sems[1].at[c, p - 1], (dp_dev(p), blk)))

    def gathered(c, buffer, sems):
        for p in range(1, n):
            arrived(buffer.at[c, share_of(dp_dev(n - p))], sems, (c, p - 1), partner)

    for c in range(CHUNKS):
        cols = slice(c * cw, (c + 1) * cw)
        partial = dot_nn(rows_low[...], data[:, cols])
        psf[c] = partial
        s_out[c] = partial.astype(bf16)
        scatter(c, s_out, s_in, sr)

    for q in range(nz):
        slot = share_of(lax.rem(zi + nz - q, nz) * CORES + 1 - core)
        arrived(x_all.at[slot], xf, q, partner)
    right_xf = x_all[...].astype(f32)
    left_xf = x_low[...].astype(f32)
    right_norm = jnp.broadcast_to(jnp.sum(right_xf * right_xf, axis=1, keepdims=True), (pairs, rows)).T
    left_norm = jnp.sum(left_xf * left_xf, axis=1, keepdims=True)
    distance = left_norm + right_norm - 2.0 * dot_nt(x_low[...], x_all[...])
    kern = jnp.exp(-0.5 * c_band * distance)
    kernel_sum = jnp.sum(kern, axis=1, keepdims=True)
    kern_low = kern.astype(bf16)
    for c in range(CHUNKS):
        cols = slice(c * cw, (c + 1) * cw)
        kx[c] = dot_nn(kern_low, x_all[:, cols])

    for c in range(CHUNKS):
        cols = slice(c * cw, (c + 1) * cw)
        score = reduced(c, s_in, sr) - part_ref[own, cols] / prior_var
        score_low = score.astype(bf16)
        s_all[c, mine, :] = score_low
        s_own[c, own, :] = score_low
        for q in range(1, nz):
            go(remote(s_all.at[c, mine], s_all.at[c, mine], sz[0].at[c, q - 1], sz[1].at[c, q - 1], (dp, z_dev(q))))
        go(remote(s_all.at[c, mine], s_all.at[c, mine], sf[0].at[c, 0], sf[1].at[c, 0], partner))
        gather(c, s_own, sa)

    def push_force(c):
        cols = slice(c * cw, (c + 1) * cw)
        for q in range(nz):
            slot = share_of(lax.rem(zi + nz - q, nz) * CORES + 1 - core)
            arrived(s_all.at[c, slot], sf, (c, q), partner)
        kernel_s = dot_nn(kern_low, s_all[c])
        ks[c] = kernel_s
        spread = kernel_sum * x_low[:, cols].astype(f32) - kx[c]
        force = (kernel_s + c_band * spread) / total
        psf[c] = force
        g_out[c] = force.astype(bf16)
        scatter(c, g_out, g_in, gr)

    for c in range(CHUNKS):
        for q in range(1, nz):
            slot = share_of(lax.rem(zi + nz - q, nz) * CORES + core)
            arrived(s_all.at[c, slot], sz, (c, q - 1), partner)
            go(remote(s_all.at[c, slot], s_all.at[c, slot], sf[0].at[c, q], sf[1].at[c, q], partner))
        if c:
            push_force(c - 1)

    push_force(CHUNKS - 1)

    for c in range(CHUNKS):
        force = reduced(c, g_in, gr)
        g_own[c] = force
        g_all[c, own, :] = force.astype(bf16)
        gather(c, g_all, ga)

    bracket = width * c_band - c_band * c_band * distance
    gram_ss = jnp.zeros((rows, pairs), f32)
    cross = jnp.zeros((rows, pairs), f32)
    left_sx = jnp.zeros((rows, 1), f32)
    right_sx = jnp.zeros((pairs, 1), f32)
    for c in range(CHUNKS):
        cols = slice(c * cw, (c + 1) * cw)
        gathered(c, s_own, sa)
        left_s, right_s = s_own[c], s_all[c]
        gram_ss += dot_nt(left_s, right_s)
        cross += dot_nt(x_low[:, cols], right_s) + dot_nt(left_s, x_all[:, cols])
        left_sx += jnp.sum(left_s.astype(f32) * x_low[:, cols].astype(f32), axis=1, keepdims=True)
        right_sx += jnp.sum(right_s.astype(f32) * x_all[:, cols].astype(f32), axis=1, keepdims=True)
    bracket += gram_ss + c_band * (left_sx - cross + jnp.broadcast_to(right_sx, (pairs, rows)).T)
    weighted = kern * bracket
    weighted_sum = jnp.sum(weighted, axis=1, keepdims=True)
    weighted_low = weighted.astype(bf16)
    for c in range(CHUNKS):
        cols = slice(c * cw, (c + 1) * cw)
        left_x = x_low[:, cols].astype(f32)
        wx = dot_nn(weighted_low, x_all[:, cols])
        spread = kernel_sum * left_x - kx[c]
        kx[c] = (
            -c_band * (weighted_sum * left_x - wx)
            + c_band * (kernel_sum * s_own[c].astype(f32) - ks[c])
            - 2.0 * c_band * c_band * spread
        ) / total

    for c in range(CHUNKS):
        gathered(c, g_all, ga)

    def project_step(t, carry):
        piece = pl.ds(pl.multiple_of(t * tile, tile), tile)
        force = jnp.concatenate([g_all[c] for c in range(CHUNKS)], axis=1)
        projected = dot_nt(force, data[piece, :])
        rows_low[:, piece] = (curv[:, piece] * projected).astype(bf16)
        return carry

    lax.fori_loop(0, TILES, project_step, 0)

    for c in range(CHUNKS):
        cols = slice(c * cw, (c + 1) * cw)
        partial = dot_nn(rows_low[...], data[:, cols]) - kx[c]
        psf[c] = partial
        o_out[c] = partial.astype(bf16)
        scatter(c, o_out, o_in, orr)

    for c in range(CHUNKS):
        value = reduced(c, o_in, orr) + g_own[c] / prior_var
        o_all[c, own, :] = value.astype(bf16)
        gather(c, o_all, oa)

    for c in range(CHUNKS):
        gathered(c, o_all, oa)
        out_ref[:, c * cw:(c + 1) * cw] = o_all[c]
    for copy in sent:
        copy.wait_send()


def solution(mesh):
    n, nb = mesh.shape["dp"], mesh.shape["blk"]
    nz = nb // CORES

    def shards(particles, data_rows, labels):
        rows, width = particles.shape
        examples = data_rows.shape[0]
        share, cw, pairs = rows // n, width // CHUNKS, rows // n * nb
        V, D = pltpu.VMEM, pltpu.SemaphoreType.DMA

        def two(*shape):
            return [D(shape), D(shape)]

        result = pl.pallas_call(
            functools.partial(kernel, n, nb),
            out_shape=jax.ShapeDtypeStruct((rows, width), bf16),
            in_specs=[pl.BlockSpec(memory_space=V), pl.BlockSpec(memory_space=V), pl.BlockSpec(memory_space=pl.ANY)],
            out_specs=pl.BlockSpec(memory_space=V),
            scratch_shapes=[
                V((examples, width), bf16),
                V((rows, examples), f32),
                V((rows, examples), bf16),
                V((rows, width), bf16),
                V((pairs, width), bf16),
                V((CHUNKS, pairs, cw), bf16),
                V((CHUNKS, rows, cw), bf16),
                V((CHUNKS, rows, cw), f32),
                V((CHUNKS, rows, cw), f32),
                V((CHUNKS, rows, cw), f32),
                V((CHUNKS, share, cw), f32),
                V((CHUNKS, rows, cw), bf16),
                V((CHUNKS, rows, cw), bf16),
                V((CHUNKS, rows, cw), bf16),
                V((CHUNKS, rows, cw), bf16),
                V((CHUNKS, rows, cw), bf16),
                V((CHUNKS, n - 1, share, cw), bf16),
                V((CHUNKS, n - 1, share, cw), bf16),
                V((CHUNKS, n - 1, share, cw), bf16),
                D((TILES,)),
                two(nz - 1),
                two(nz),
                two(CHUNKS, n - 1),
                two(CHUNKS, n - 1),
                two(CHUNKS, nz - 1),
                two(CHUNKS, nz),
                two(CHUNKS, n - 1),
                two(CHUNKS, n - 1),
                two(CHUNKS, n - 1),
                two(CHUNKS, n - 1),
            ],
            compiler_params=pltpu.CompilerParams(
                collective_id=0, has_side_effects=True, vmem_limit_bytes=56 * 1024 * 1024
            ),
        )(particles, labels.reshape(1, examples), data_rows)
        return result.astype(f32)

    placed = (P("blk", None), P("dp", None), P("dp"))
    return jax.shard_map(shards, mesh=mesh, in_specs=placed, out_specs=P("blk", None), check_vma=False)
```
